128 devices in a mesh: member: 16 (over y_hi, z, core), dp: 8 (over x, y_lo).
Axes of the slice: x: 4, y: 4 (y_hi: 2, y_lo: 2; y = y_hi * 2 + y_lo), z: 4, core: 2. Of those that a mesh axis runs over, the one named last changes fastest.
Arguments:
- feats: bfloat16 [16, 4096, 1024], P('member', 'dp'), may hold values from -160 to 160
- pair_weight: float32 [16, 3], replicated, may hold values from 0.5 to 2
Outputs:
- grad_centred: float32 [16, 4096, 1024], P('member', 'dp')
- cka: float32 [16, 3], P('member')
The draws below stay inside these ranges and needn't reach their ends.
All inputs are finite; a program needn't handle non-finite values.
Results may differ from the reference program's by a relative error of at most 0.0053.
Values may be sent and summed in bfloat16 or wider, within the bound.
No kernel may reach another device: no remote copies, remote signals or barrier semaphores. Data moves between devices by JAX's collectives and lax.ppermute only.
A program may use at most 128 MiB of HBM per device.

```python
import math
import jax
import jax.numpy as jnp
from jax import lax

F = 1024
PAIRS = 3
BATCH = 4096
MEMBERS = 16


def draw_feats(key, part):
    keys = jax.random.split(jax.random.fold_in(key, 71), 4)
    shape = (MEMBERS, BATCH, F)
    noise = jnp.clip(jax.random.normal(keys[0], shape, jnp.float32), -5.0, 5.0)
    position = jnp.arange(BATCH, dtype=jnp.float32) / BATCH
    ramp = (3.0 ** position)[None, :, None] / 3.0
    row_scale = ramp * 10.0 ** jax.random.uniform(keys[1], (MEMBERS, BATCH, 1), jnp.float32, 0.0, 1.0)
    col_scale = 10.0 ** jax.random.uniform(keys[2], (MEMBERS, 1, F), jnp.float32, -0.5, 0.5)
    offset = jax.random.uniform(keys[3], (MEMBERS, 1, F), jnp.float32, -1.5, 1.5)
    return (row_scale * col_scale * noise + offset).astype(jnp.bfloat16)


def setup_inputs(seed: int = 0) -> dict:
    key_of = jax.random.split(jax.random.key(seed), 3)
    return {
        "feats": draw_feats(jax.random.fold_in(key_of[2], 71), 0),
        "pair_weight": jnp.clip(jnp.exp(jax.random.uniform(key_of[1], (MEMBERS, PAIRS), jnp.float32, math.log(0.5), math.log(2.0))), 0.5, 2.0),
    }


def reference(feats, pair_weight):
    members = feats.shape[0]
    batch = feats.shape[1]
    mean = lax.optimization_barrier(jnp.sum(feats.astype(jnp.float32), axis=1, keepdims=True)) / batch
    centred = (feats.astype(jnp.float32) - mean).astype(jnp.bfloat16)
    covs = []
    for member in range(members):
        row = []
        for offset in range(PAIRS + 1):
            partner = (member + offset) % members
            row.append(jnp.dot(centred[member].T, centred[partner], preferred_element_type=jnp.float32))
        covs.append(row)
    hself = jnp.stack([jnp.sum(covs[m][0] * covs[m][0]) for m in range(members)])
    hpair = jnp.stack([jnp.stack([jnp.sum(covs[m][o] * covs[m][o]) for o in range(1, PAIRS + 1)]) for m in range(members)])
    partner_self = jnp.stack([jnp.roll(hself, -o) for o in range(1, PAIRS + 1)], axis=1)
    norms = jnp.sqrt(hself[:, None] * partner_self)
    cka = hpair / norms
    weighted = pair_weight * cka
    mixers = []
    for member in range(members):
        mixers.append([(2.0 * pair_weight[member, o - 1] / norms[member, o - 1] * covs[member][o]).astype(jnp.bfloat16) for o in range(1, PAIRS + 1)])
    grads = []
    for member in range(members):
        incoming = jnp.float32(0.0)
        for o in range(1, PAIRS + 1):
            incoming = incoming + weighted[(member - o) % members, o - 1]
        self_coef = (jnp.sum(weighted[member]) + incoming) / (hself[member] + 1e-06)
        self_mix = (2.0 * self_coef * covs[member][0]).astype(jnp.bfloat16)
        total = -jnp.dot(centred[member], self_mix, preferred_element_type=jnp.float32)
        for o in range(1, PAIRS + 1):
            total = total + jnp.dot(centred[(member + o) % members], mixers[member][o - 1].T, preferred_element_type=jnp.float32)
            source = (member - o) % members
            total = total + jnp.dot(centred[source], mixers[source][o - 1], preferred_element_type=jnp.float32)
        grads.append(math.sqrt(batch) * total)
    return (jnp.stack(grads), cka)
```

```python
import math

import jax
import jax.numpy as jnp
from jax import lax
from jax.sharding import Mesh
from jax.sharding import PartitionSpec as P

DP = ("dp_0", "dp_1")
PARTNERS = (1, 2, -3)


def of_everyone(value, axis):
    copies = jnp.broadcast_to(value, (lax.axis_size(axis), *value.shape))
    return lax.all_to_all(copies, axis, split_axis=0, concat_axis=0, tiled=True)


def moved(value, axis, steps):
    count = lax.axis_size(axis)
    pairs = [(source, (source + steps) % count) for source in range(count)]
    return lax.ppermute(value, axis, pairs)


def wide_dot(a, b, dims):
    return lax.dot_general(a, b, (dims, ((), ())), preferred_element_type=jnp.float32)


def shards(feats, pair_weight):
    rows = feats[0]
    height, width = rows.shape
    around = lax.axis_size("dp_0")
    batch = height * lax.axis_size(DP)
    block = width // around
    x = lax.axis_index("dp_0")
    y = lax.axis_index("dp_1")
    member = lax.axis_index("member")
    count = len(PARTNERS) + 1

    def columns(value, index):
        return lax.dynamic_slice_in_dim(value, index * block, block, axis=value.ndim - 1)

    own_blocks = [columns(rows, x)]
    for d in range(1, around):
        own_blocks.append(moved(columns(rows, (x - d) % around), "dp_0", -d))
    own_block = jnp.concatenate(own_blocks, axis=0)
    partner_blocks = [moved(own_block, "member", -o) for o in PARTNERS]
    wide_rows = jnp.concatenate([rows] + [moved(rows, "dp_0", -d) for d in range(1, around)], axis=0)

    totals = jnp.sum(of_everyone(jnp.sum(rows.astype(jnp.float32), axis=0), DP), axis=0)
    mean = totals / batch
    block_mean = columns(mean, x)
    means = [block_mean] + [moved(block_mean, "member", -o) for o in PARTNERS]
    centred = (wide_rows.astype(jnp.float32) - mean).astype(jnp.bfloat16)
    blocks = [
        (b.astype(jnp.float32) - mu).astype(jnp.bfloat16)
        for b, mu in zip([own_block] + partner_blocks, means)
    ]

    covs = []
    for b in blocks:
        part = wide_dot(centred, b, ((0,), (0,)))
        other = moved(part.astype(jnp.bfloat16), "dp_1", 1)
        covs.append(part + other.astype(jnp.float32))

    returned = [
        moved(wide_dot(centred, c.astype(jnp.bfloat16), ((1,), (0,))).astype(jnp.bfloat16), "member", o)
        for c, o in zip(covs[1:], PARTNERS)
    ]

    half = width // 2
    squares = []
    for c in covs:
        mine = lax.dynamic_slice_in_dim(c, y * half, half, axis=0)
        squares.append(jnp.sum(mine * mine))
    sums = jnp.sum(of_everyone(jnp.stack(squares), DP), axis=0)
    table = of_everyone(sums, "member")
    hself = table[:, 0]
    hpair = jnp.stack([jnp.roll(table[:, k], min(o, 0)) for k, o in enumerate(PARTNERS, 1)], axis=1)
    partner_self = jnp.stack([jnp.roll(hself, -abs(o)) for o in PARTNERS], axis=1)
    norms = jnp.sqrt(hself[:, None] * partner_self)
    cka = hpair / norms
    weighted = pair_weight * cka
    incoming = jnp.stack([jnp.roll(weighted[:, k], abs(o)) for k, o in enumerate(PARTNERS)], axis=1)
    self_coef = (jnp.sum(weighted, axis=1) + jnp.sum(incoming, axis=1)) / (hself + 1e-06)
    pair_coef = 2.0 * pair_weight / norms
    held = [jnp.roll(pair_coef[:, k], -min(o, 0)) for k, o in enumerate(PARTNERS)]
    back = [jnp.roll(h, o) for h, o in zip(held, PARTNERS)]
    factors = jnp.stack([-2.0 * self_coef] + held + back, axis=1)
    both = jnp.concatenate([factors, cka], axis=1)
    chosen = (jnp.arange(both.shape[0], dtype=jnp.int32) == member)[:, None]
    own = jnp.sum(jnp.where(chosen, both, 0.0), axis=0)
    own_cka = own[2 * count - 1 :]

    mixers = jnp.concatenate([(own[k] * covs[k]).astype(jnp.bfloat16) for k in range(count)], axis=1)
    local = wide_dot(jnp.concatenate(blocks, axis=1), mixers, ((1,), (1,)))
    local = local.reshape(around, height, width)
    total = local[0]
    for d in range(1, around):
        total = total + moved(local[d].astype(jnp.bfloat16), "dp_0", d).astype(jnp.float32)

    back_sum = sum(own[count + k] * returned[k].astype(jnp.float32) for k in range(count - 1))
    back_sum = back_sum.reshape(around, height, block)
    pieces = [back_sum[0]]
    for d in range(1, around):
        pieces.append(moved(back_sum[d].astype(jnp.bfloat16), "dp_0", d).astype(jnp.float32))
    ordered = jnp.concatenate(pieces[::-1] + pieces[:0:-1], axis=1)
    ordered = lax.dynamic_slice_in_dim(ordered, (around - 1 - x) * block, width, axis=1)
    grad = math.sqrt(batch) * (total + ordered)
    return (grad[None], own_cka[None])


def solution(mesh):
    finer = Mesh(mesh.devices.reshape(mesh.shape["member"], 4, 2), ("member", "dp_0", "dp_1"))
    return jax.shard_map(
        shards,
        mesh=finer,
        in_specs=(P("member", DP, None), P()),
        out_specs=(P("member", DP, None), P("member", None)),
        check_vma=False,
    )
```

```python
import math

import jax
import jax.numpy as jnp
from jax import lax
from jax.sharding import Mesh
from jax.sharding import PartitionSpec as P

DP = ("dp_0", "dp_1")


def of_everyone(value, axis):
    copies = jnp.broadcast_to(value, (lax.axis_size(axis), *value.shape))
    return lax.all_to_all(copies, axis, split_axis=0, concat_axis=0, tiled=True)


def moved(value, axis, steps):
    count = lax.axis_size(axis)
    return lax.ppermute(value, axis, [(s, (s + steps) % count) for s in range(count)])


def moved_some(value, first, steps):
    count = lax.axis_size("member")
    return lax.ppermute(value, "member", [(s, (s + steps) % count) for s in range(first, count, 2)])


def swapped(value):
    return lax.ppermute(value, "member", [(s, s ^ 1) for s in range(lax.axis_size("member"))])


def crossing(value, from_even, from_odd):
    count = lax.axis_size("member")
    pairs = [(s, (s + (from_odd if s % 2 else from_even)) % count) for s in range(count)]
    return lax.ppermute(value, "member", pairs)


def after(value, *others):
    return lax.optimization_barrier((value, others))[0]


def wide_dot(a, b, left, right):
    return lax.dot_general(a, b, (((left,), (right,)), ((), ())), preferred_element_type=jnp.float32)


def f32(value):
    return value.astype(jnp.float32)


def bf16(value):
    return value.astype(jnp.bfloat16)


def body(feats, pair_weight):
    rows = feats[0]
    height, width = rows.shape
    around = lax.axis_size("dp_0")
    batch = height * lax.axis_size(DP)
    block = width // around
    half = width // 2
    x = lax.axis_index("dp_0")
    member = lax.axis_index("member")
    even = member % 2 == 0
    cut = (slice(0, half), slice(half, width))

    def columns(value, index):
        return lax.dynamic_slice_in_dim(value, index * block, block, axis=value.ndim - 1)

    mean = jnp.sum(of_everyone(jnp.sum(f32(rows), axis=0), DP), axis=0) / batch

    own = [columns(rows, x)]
    for d in range(1, around):
        own.append(moved(columns(rows, (x - d) % around), "dp_0", -d))
    block_mean = columns(mean, x)
    own = jnp.concatenate([bf16(f32(o) - block_mean) for o in own], axis=0)

    second = moved(own, "member", -2)
    crossed = swapped(second)
    step = moved(own, "member", 1)
    far = moved_some(step, 0, 2)
    third = jnp.where(even, far, step)
    blocks = [own, second, crossed, third]

    h0, h1 = rows[: height // 2], rows[height // 2 :]
    p0 = moved(h0, "dp_0", 1)
    m0 = moved(h0, "dp_0", -1)
    m1 = moved(h1, "dp_0", -1)
    p1 = moved(h1, "dp_0", 1)
    f0 = moved(p0, "dp_0", 1)
    f1 = moved(m1, "dp_0", -1)
    centred = jnp.concatenate([bf16(f32(v) - mean) for v in (h0, h1, m0, m1, f0, f1, p0, p1)], axis=0)

    def pair_sum(k):
        part = bf16(wide_dot(centred, blocks[k], 0, 0))
        return f32(part) + f32(moved(part, "dp_1", 1))

    covs = [pair_sum(k) for k in range(4)]

    def over_ring(value, first=(), second=()):
        for bit, others in ((1, first), (2, second)):
            come = lax.ppermute(value, "dp_0", [(s, s ^ bit) for s in range(around)])
            value = value + after(come, *others)
        return value

    def square_rows(ks):
        lines = jnp.arange(8)[:, None]
        return sum(jnp.where(lines == k, jnp.sum(covs[k] * covs[k], axis=0)[None], 0.0) for k in ks)

    def filled(lines):
        ones = jnp.ones((block, block), jnp.float32)
        return lax.dot_general(lines, ones, (((1,), (0,)), ((), ())), precision=lax.Precision.HIGHEST)

    members, pairs = pair_weight.shape

    def either(a, b):
        return jnp.where(even, a, b)

    wanted = (
        (member, 1),
        (member, either(2, 0)),
        (either(member - 3, member - 1), either(2, 0)),
        (member, 0),
        (member, 2),
        (member - 2, 1),
        (member - 1, 0),
        (member - 3, 2),
    )
    places = jnp.stack([(q % members) * pairs + column for q, column in wanted])
    picked = (jnp.arange(members * pairs)[None] == places[:, None]).astype(jnp.float32)
    weights = jnp.sum(picked * pair_weight.reshape(1, -1), axis=1, keepdims=True)
    weights = lax.optimization_barrier(jnp.broadcast_to(weights, (len(wanted), block)))
    weights = [weights[i : i + 1] for i in range(len(wanted))]

    hself = filled(over_ring(square_rows((0,))))
    h_p2 = moved(hself, "member", -2)
    h_s2 = crossing(hself, -1, -3)
    h_s3 = crossing(hself, 1, 3)
    hself, h_p2, h_s2, h_s3 = (v[:1] for v in (hself, h_p2, h_s2, h_s3))

    coefs = [2.0 * w / jnp.sqrt(hself * h) for w, h in zip(weights, (h_p2, h_s2, h_s3))]
    coefs = lax.optimization_barrier(coefs)
    mixer = {k: bf16(coefs[k - 1] * covs[k]) for k in (1, 2, 3)}
    mixers = jnp.concatenate([mixer[k] for k in (1, 2, 3)], axis=1)

    partners = jnp.concatenate(blocks[1:], axis=1)

    def share(d, h):
        return wide_dot(partners[d * height : (d + 1) * height], mixers[cut[h]], 1, 1)

    def own_share():
        return wide_dot(partners[:height], mixers, 1, 1)

    def outgoing(cov):
        return wide_dot(centred, cov, 1, 0)

    out3 = bf16(outgoing(mixer[3]))
    near = moved(out3, "member", -1)
    out2 = bf16(outgoing(mixer[2]))
    out2 = swapped(out2)
    back3 = jnp.where(even, near, moved_some(near, 1, -2))
    a0 = moved(bf16(share(2, 0)), "dp_0", 1)
    c0 = moved(bf16(share(3, 0)), "dp_0", -1)
    out1 = bf16(outgoing(mixer[1]) + f32(out2))
    back1 = moved(out1, "member", 2)
    a1 = moved(bf16(share(2, 1)), "dp_0", -1)
    c1_sent = bf16(share(1, 1))
    c1 = moved(c1_sent, "dp_0", 1)
    b0 = bf16(share(1, 0) + f32(a0))
    b0 = moved(b0, "dp_0", 1)
    self_term = bf16(outgoing(bf16(covs[0]))).reshape(around, height, block)
    self_parts = [self_term[0]] + [moved(self_term[d], "dp_0", d) for d in range(1, around)]
    b1_sent = bf16(share(3, 1) + f32(a1))
    b1 = moved(b1_sent, "dp_0", -1)
    sums = filled(over_ring(square_rows((1, 2, 3)), (c1_sent,), (b1_sent,)))
    sums, hself, h_p2, h_s2, h_s3 = lax.optimization_barrier((sums, hself, h_p2, h_s2, h_s3))
    cka2 = sums[1:2] / jnp.sqrt(hself * h_p2)
    held2 = sums[2:3] / jnp.sqrt(hself * h_s2)
    held3 = sums[3:4] / jnp.sqrt(h_s3 * hself)
    lines = jnp.arange(8)[:, None]
    ckas = jnp.where(lines == 1, cka2, jnp.where(lines == 2, held2, held3))
    own_part = weights[0] * cka2
    own_part = own_part + either(weights[4], weights[3]) * held2 + either(weights[7], weights[6]) * held3
    ckas, own_part, scale = lax.optimization_barrier((ckas, own_part, -2.0 / (hself + 1e-06)))
    back = f32(back1) + f32(back3)
    back = back.reshape(around, height, block)
    back_sent = [bf16(back[d]) for d in range(1, around)]
    back_parts = [back[0]] + [f32(moved(v, "dp_0", d)) for d, v in enumerate(back_sent, 1)]
    arrived = after((b0, c0, b1, c1), *back_sent)
    local = own_share() + jnp.concatenate(
        [f32(arrived[0]) + f32(arrived[1]), f32(arrived[2]) + f32(arrived[3])], axis=1
    )
    come1 = after(moved(ckas, "member", 2), *back_sent)[1:2]
    come3 = after(crossing(ckas, -3, -1), *back_sent)[3:4]
    come2 = after(crossing(ckas, 3, 1), *back_sent)[2:3]
    total = own_part + weights[5] * come1
    total = total + either(weights[3], weights[4]) * come3 + either(weights[6], weights[7]) * come2
    self_coef = scale * total
    cka2, held2 = ckas[1:2], ckas[2:3]
    cka1, cka3 = either(come3, held2), either(held2, come3)
    lane = jnp.arange(pairs)[None]
    cka = jnp.where(lane == 0, cka1[:, :pairs], jnp.where(lane == 1, cka2[:, :pairs], cka3[:, :pairs]))

    pieces = [p + self_coef * f32(q) for p, q in zip(back_parts, self_parts)]
    parts = []
    for b in range(around):
        come = pieces[0]
        for d in range(1, around):
            come = jnp.where((x - b) % around == d, pieces[d], come)
        parts.append(math.sqrt(batch) * (local[:, b * block : (b + 1) * block] + come))
    grad = jnp.concatenate(parts, axis=1)
    return (grad[None], cka)


def solution(mesh):
    finer = Mesh(mesh.devices.reshape(mesh.shape["member"], 4, 2), ("member", "dp_0", "dp_1"))
    return jax.shard_map(
        body,
        mesh=finer,
        in_specs=(P("member", DP, None), P()),
        out_specs=(P("member", DP, None), P("member", None)),
        check_vma=False,
    )
```

```python
import math

import jax
import jax.numpy as jnp
from jax import lax
from jax.sharding import Mesh
from jax.sharding import PartitionSpec as P

DP = ("dp_0", "dp_1")


def of_everyone(value, axis):
    copies = jnp.broadcast_to(value, (lax.axis_size(axis), *value.shape))
    return lax.all_to_all(copies, axis, split_axis=0, concat_axis=0, tiled=True)


def moved(value, axis, steps):
    count = lax.axis_size(axis)
    return lax.ppermute(value, axis, [(s, (s + steps) % count) for s in range(count)])


def moved_some(value, first, steps):
    count = lax.axis_size("member")
    return lax.ppermute(value, "member", [(s, (s + steps) % count) for s in range(first, count, 2)])


def swapped(value):
    return lax.ppermute(value, "member", [(s, s ^ 1) for s in range(lax.axis_size("member"))])


def crossing(value, from_even, from_odd):
    count = lax.axis_size("member")
    pairs = [(s, (s + (from_odd if s % 2 else from_even)) % count) for s in range(count)]
    return lax.ppermute(value, "member", pairs)


def after(value, *others):
    return lax.optimization_barrier((value, others))[0]


def wide_dot(a, b, left, right):
    return lax.dot_general(a, b, (((left,), (right,)), ((), ())), preferred_element_type=jnp.float32)


def f32(value):
    return value.astype(jnp.float32)


def bf16(value):
    return value.astype(jnp.bfloat16)


def body(feats, pair_weight):
    rows = feats[0]
    height, width = rows.shape
    around = lax.axis_size("dp_0")
    batch = height * lax.axis_size(DP)
    block = width // around
    half = width // 2
    x = lax.axis_index("dp_0")
    member = lax.axis_index("member")
    even = member % 2 == 0
    cut = (slice(0, half), slice(half, width))

    def columns(value, index):
        return lax.dynamic_slice_in_dim(value, index * block, block, axis=value.ndim - 1)

    mean = jnp.sum(of_everyone(jnp.sum(f32(rows), axis=0), DP), axis=0) / batch

    own = [columns(rows, x)]
    for d in range(1, around):
        own.append(moved(columns(rows, (x - d) % around), "dp_0", -d))
    block_mean = columns(mean, x)
    own = jnp.concatenate([bf16(f32(o) - block_mean) for o in own], axis=0)

    second = moved(own, "member", -2)
    crossed = swapped(second)
    step = moved(own, "member", 1)
    far = moved_some(step, 0, 2)
    third = jnp.where(even, far, step)
    blocks = [own, second, crossed, third]

    h0, h1 = rows[: height // 2], rows[height // 2 :]
    p0 = moved(h0, "dp_0", 1)
    m0 = moved(h0, "dp_0", -1)
    m1 = moved(h1, "dp_0", -1)
    p1 = moved(h1, "dp_0", 1)
    f0 = moved(p0, "dp_0", 1)
    f1 = moved(m1, "dp_0", -1)
    centred = jnp.concatenate([bf16(f32(v) - mean) for v in (h0, h1, m0, m1, f0, f1, p0, p1)], axis=0)

    def pair_sum(k):
        part = bf16(wide_dot(centred, blocks[k], 0, 0))
        return f32(part) + f32(moved(part, "dp_1", 1))

    covs = [pair_sum(k) for k in range(4)]

    def over_ring(value, first=(), second=()):
        for bit, others in ((1, first), (2, second)):
            come = lax.ppermute(value, "dp_0", [(s, s ^ bit) for s in range(around)])
            value = value + after(come, *others)
        return value

    def square_rows(ks):
        lines = jnp.arange(8)[:, None]
        return sum(jnp.where(lines == k, jnp.sum(covs[k] * covs[k], axis=0)[None], 0.0) for k in ks)

    def filled(lines):
        ones = jnp.ones((block, block), jnp.float32)
        return lax.dot_general(lines, ones, (((1,), (0,)), ((), ())), precision=lax.Precision.HIGHEST)

    members, pairs = pair_weight.shape

    def either(a, b):
        return jnp.where(even, a, b)

    wanted = (
        (member, 1),
        (member, either(2, 0)),
        (either(member - 3, member - 1), either(2, 0)),
        (member, 0),
        (member, 2),
        (member - 2, 1),
        (member - 1, 0),
        (member - 3, 2),
    )
    places = jnp.stack([(q % members) * pairs + column for q, column in wanted])
    picked = (jnp.arange(members * pairs)[None] == places[:, None]).astype(jnp.float32)
    weights = jnp.sum(picked * pair_weight.reshape(1, -1), axis=1, keepdims=True)
    weights = lax.optimization_barrier(jnp.broadcast_to(weights, (len(wanted), block)))
    weights = [weights[i : i + 1] for i in range(len(wanted))]

    hself = filled(over_ring(square_rows((0,))))
    h_p2 = moved(hself, "member", -2)
    h_s2 = crossing(hself, -1, -3)
    h_s3 = crossing(hself, 1, 3)
    hself, h_p2, h_s2, h_s3 = (v[:1] for v in (hself, h_p2, h_s2, h_s3))

    coefs = [2.0 * w / jnp.sqrt(hself * h) for w, h in zip(weights, (h_p2, h_s2, h_s3))]
    coefs = lax.optimization_barrier(coefs)
    mixer = {k: bf16(coefs[k - 1] * covs[k]) for k in (1, 2, 3)}
    mixers = jnp.concatenate([mixer[k] for k in (1, 2, 3)], axis=1)

    partners = jnp.concatenate(blocks[1:], axis=1)

    def share(d, h):
        return wide_dot(partners[d * height : (d + 1) * height], mixers[cut[h]], 1, 1)

    def own_share():
        return wide_dot(partners[:height], mixers, 1, 1)

    def outgoing(cov):
        return wide_dot(centred, cov, 1, 0)

    out3 = bf16(outgoing(mixer[3]))
    near = moved(out3, "member", -1)
    out2 = bf16(outgoing(mixer[2]))
    out2 = swapped(out2)
    back3 = jnp.where(even, near, moved_some(near, 1, -2))
    a0 = moved(bf16(share(2, 0)), "dp_0", 1)
    c0 = moved(bf16(share(3, 0)), "dp_0", -1)
    out1 = bf16(outgoing(mixer[1]) + f32(out2))
    back1 = moved(out1, "member", 2)
    a1 = moved(bf16(share(2, 1)), "dp_0", -1)
    c1_sent = bf16(share(1, 1))
    c1 = moved(c1_sent, "dp_0", 1)
    b0 = bf16(share(1, 0) + f32(a0))
    b0 = moved(b0, "dp_0", 1)
    self_term = bf16(outgoing(bf16(covs[0]))).reshape(around, height, block)
    self_parts = [self_term[0]] + [moved(self_term[d], "dp_0", d) for d in range(1, around)]
    b1_sent = bf16(share(3, 1) + f32(a1))
    b1 = moved(b1_sent, "dp_0", -1)
    sums = filled(over_ring(square_rows((1, 2, 3)), (c1_sent,), (b1_sent,)))
    sums, hself, h_p2, h_s2, h_s3 = lax.optimization_barrier((sums, hself, h_p2, h_s2, h_s3))
    cka2 = sums[1:2] / jnp.sqrt(hself * h_p2)
    held2 = sums[2:3] / jnp.sqrt(hself * h_s2)
    held3 = sums[3:4] / jnp.sqrt(h_s3 * hself)
    lines = jnp.arange(8)[:, None]
    ckas = jnp.where(lines == 1, cka2, jnp.where(lines == 2, held2, held3))
    own_part = weights[0] * cka2
    own_part = own_part + either(weights[4], weights[3]) * held2 + either(weights[7], weights[6]) * held3
    ckas, own_part, scale = lax.optimization_barrier((ckas, own_part, -2.0 / (hself + 1e-06)))
    back = f32(back1) + f32(back3)
    back = back.reshape(around, height, block)
    back_sent = [bf16(back[d]) for d in range(1, around)]
    back_parts = [back[0]] + [f32(moved(v, "dp_0", d)) for d, v in enumerate(back_sent, 1)]
    arrived = after((b0, c0, b1, c1), *back_sent)
    local = own_share() + jnp.concatenate(
        [f32(arrived[0]) + f32(arrived[1]), f32(arrived[2]) + f32(arrived[3])], axis=1
    )
    come1 = after(moved(ckas, "member", 2), *back_sent)[1:2]
    come3 = after(crossing(ckas, -3, -1), *back_sent)[3:4]
    come2 = after(crossing(ckas, 3, 1), *back_sent)[2:3]
    total = own_part + weights[5] * come1
    total = total + either(weights[3], weights[4]) * come3 + either(weights[6], weights[7]) * come2
    self_coef = scale * total
    cka2, held2 = ckas[1:2], ckas[2:3]
    cka1, cka3 = either(come3, held2), either(held2, come3)
    lane = jnp.arange(pairs)[None]
    cka = jnp.where(lane == 0, cka1[:, :pairs], jnp.where(lane == 1, cka2[:, :pairs], cka3[:, :pairs]))

    parts = []
    for b in range(around):
        come, own_come = back_parts[0], self_parts[0]
        for d in range(1, around):
            here = (x - b) % around == d
            come = jnp.where(here, back_parts[d], come)
            own_come = jnp.where(here, self_parts[d], own_come)
        come = come + self_coef * f32(own_come)
        parts.append(math.sqrt(batch) * (local[:, b * block : (b + 1) * block] + come))
    grad = jnp.concatenate(parts, axis=1)
    return (grad[None], cka)


def solution(mesh):
    finer = Mesh(mesh.devices.reshape(mesh.shape["member"], 4, 2), ("member", "dp_0", "dp_1"))
    return jax.shard_map(
        body,
        mesh=finer,
        in_specs=(P("member", DP, None), P()),
        out_specs=(P("member", DP, None), P("member", None)),
        check_vma=False,
    )
```
